512 devices in a mesh: rows: 512 (over z, y, x, core).
Axes of the slice: x: 4, y: 8, z: 8, core: 2. Of those that a mesh axis runs over, the one named last changes fastest.
Arguments:
- adj_diag: int32 [8192, 512], P('rows'), may hold values from -2147483648 to 2147483647
- adj_right: int32 [8192, 512], P('rows'), may hold values from -2147483648 to 2147483647
- alive_diag: int32 [8192, 512], P('rows'), may hold values from -2147483648 to 2147483647
- alive_right: int32 [8192, 512], P('rows'), may hold values from -2147483648 to 2147483647
- truss_k: int32 [1], replicated, may hold values from 130 to 193
Outputs:
- support_field: float32 [262144, 1024], P('rows')
- removed_counts: int32 [3], replicated
The draws below stay inside these ranges and needn't reach their ends.
All inputs are finite; a program needn't handle non-finite values.
Results may differ from the reference program's by a relative error of at most 0.0003.
Values may be sent and summed in bfloat16 or wider, within the bound.
A program may use at most 64 MiB of HBM per device.

```python
import jax
import jax.numpy as jnp
from jax import lax

TILE = 512
ITERS = 3
NVERT = 262144


def vertex_levels(key, block):
    base_key = jax.random.fold_in(jax.random.fold_in(key, 7001), block)
    size_key, order_key, level_key = jax.random.split(base_key, 3)
    core_count = jax.random.randint(size_key, (), TILE // 4, 3 * TILE // 8 + 1, dtype=jnp.int32)
    order = jax.random.permutation(order_key, TILE)
    is_core = order < core_count
    levels = jax.random.randint(level_key, (TILE,), 2, 16, dtype=jnp.int32)
    return (jnp.where(is_core, jnp.int32(16), levels), is_core)


def pack_bits(tile_bits):
    shifts = jnp.arange(32, dtype=jnp.int32)
    sectioned = tile_bits.reshape(TILE // 32, 32, TILE)
    return jnp.sum(sectioned << shifts[None, :, None], axis=1, dtype=jnp.int32)


def draw_bits(key, salt, offset, alive_kind):
    blocks = NVERT // TILE

    def one_block(block):
        row_levels, row_core = vertex_levels(key, block)
        col_levels, col_core = vertex_levels(key, (block + offset) % blocks)
        edge_key = jax.random.fold_in(jax.random.fold_in(key, salt), block)
        if alive_kind:
            chance = jax.random.randint(edge_key, (TILE, TILE), 0, 8, dtype=jnp.int32)
            both_core = row_core[:, None] & col_core[None, :]
            tile_bits = jnp.where(both_core, jnp.int32(1), (chance < 7).astype(jnp.int32))
        else:
            chance = jax.random.randint(edge_key, (TILE, TILE), 0, 256, dtype=jnp.int32)
            tile_bits = (chance < row_levels[:, None] * col_levels[None, :]).astype(jnp.int32)
        return pack_bits(tile_bits)
    packed = lax.map(one_block, jnp.arange(blocks, dtype=jnp.int32))
    return packed.reshape(NVERT // 32, TILE)


def draw_adj_diag(key, part):
    return draw_bits(key, 101, 0, False)


def draw_adj_right(key, part):
    return draw_bits(key, 102, 1, False)


def draw_alive_diag(key, part):
    return draw_bits(key, 103, 0, True)


def draw_alive_right(key, part):
    return draw_bits(key, 104, 1, True)


def setup_inputs(seed: int = 0) -> dict:
    seeds = jax.random.split(jax.random.key(seed), 6)
    adj_diag = draw_adj_diag(jax.random.fold_in(seeds[5], 71), 0)
    adj_right = draw_adj_right(jax.random.fold_in(seeds[5], 71), 0)
    alive_diag = draw_alive_diag(jax.random.fold_in(seeds[5], 71), 0)
    alive_right = draw_alive_right(jax.random.fold_in(seeds[5], 71), 0)
    truss_k = jax.random.randint(seeds[4], (1,), TILE // 4 + 2, 3 * TILE // 8 + 2).astype(jnp.int32)
    return {"adj_diag": adj_diag, "adj_right": adj_right, "alive_diag": alive_diag, "alive_right": alive_right, "truss_k": truss_k}


def unpack_tiles(packed, blocks, tile):
    shifts = jnp.arange(32, dtype=jnp.int32)
    sectioned = packed.reshape(blocks, tile // 32, tile)
    tile_bits = (sectioned[:, :, None, :] >> shifts[None, None, :, None]) & 1
    return tile_bits.reshape(blocks, tile, tile)


def tile_support(pieces):
    within, across, prev_across, next_within = pieces
    inside = lax.dot_general(prev_across, prev_across, (((0,), (0,)), ((), ())), preferred_element_type=jnp.float32)
    inside = inside + jnp.dot(within, within, preferred_element_type=jnp.float32)
    inside = inside + lax.dot_general(across, across, (((1,), (1,)), ((), ())), preferred_element_type=jnp.float32)
    between = jnp.dot(within, across, preferred_element_type=jnp.float32)
    between = between + jnp.dot(across, next_within, preferred_element_type=jnp.float32)
    return inside, between


def reference(adj_diag, adj_right, alive_diag, alive_right, truss_k):
    blocks = NVERT // TILE
    upper_half = jnp.triu(unpack_tiles(adj_diag & alive_diag, blocks, TILE), 1)
    within = (upper_half + jnp.swapaxes(upper_half, 1, 2)).astype(jnp.bfloat16)
    across = unpack_tiles(adj_right & alive_right, blocks, TILE).astype(jnp.bfloat16)
    thresh = (truss_k[0] - 2).astype(jnp.float32)
    counts = []
    for step in range(ITERS):
        prev_across = jnp.roll(across, 1, axis=0)
        next_within = jnp.roll(within, -1, axis=0)
        inside, between = lax.map(tile_support, (within, across, prev_across, next_within))
        new_within = jnp.where(inside >= thresh, within, jnp.zeros_like(within))
        new_across = jnp.where(between >= thresh, across, jnp.zeros_like(across))
        lost_within = jnp.sum((within - new_within).astype(jnp.int32)) // 2
        lost_across = jnp.sum((across - new_across).astype(jnp.int32))
        counts.append(lost_within + lost_across)
        within, across = new_within, new_across
    support = jnp.concatenate([inside * within.astype(jnp.float32), between * across.astype(jnp.float32)], axis=2)
    return support.reshape(NVERT, 2 * TILE), jnp.stack(counts).astype(jnp.int32)
```

```python
import functools

import jax
import jax.numpy as jnp
from jax import lax
from jax.experimental import pallas as pl
from jax.experimental.pallas import tpu as pltpu
from jax.sharding import PartitionSpec as P

MESH = pl.DeviceIdType.MESH
AXIS = "rows"
WORD = 32
STAGES = {512: ((1, 8), (8, 8), (64, 8)), 16: ((1, 4), (4, 4))}
HALO = (1, -1, 2, -2)


def upper_words(words):
    row = lax.broadcasted_iota(jnp.int32, words.shape, 0)
    col = lax.broadcasted_iota(jnp.int32, words.shape, 1)
    ahead = col - WORD * row
    low_bits = (jnp.int32(1) << jnp.clip(ahead, 0, WORD - 1)) - 1
    return words & jnp.where(ahead >= WORD, jnp.int32(-1), low_bits)


def unpack(words_ref, out_ref, dtype):
    width = words_ref.shape[1]
    bit = lax.broadcasted_iota(jnp.int32, (WORD, width), 0)
    for w in range(words_ref.shape[0]):
        bits = (jnp.broadcast_to(words_ref[w : w + 1, :], (WORD, width)) >> bit) & 1
        out_ref[w * WORD : (w + 1) * WORD, :] = bits.astype(jnp.float32).astype(dtype)


def dot(a, b, a_dim, b_dim):
    return lax.dot_general(
        a, b, (((a_dim,), (b_dim,)), ((), ())), preferred_element_type=jnp.float32
    )


def kernel(
    ndev, tile,
    adj_diag, adj_right, alive_diag, alive_right, truss_k,
    support, counts,
    staged, k_smem, mine, near, far, wide, across, slots,
    in_sem, k_sem, send_sem, recv_sem, sum_send, sum_recv,
):
    stages = STAGES[ndev]
    words = tile // WORD
    me = lax.axis_index(AXIS)
    loads = [
        pltpu.make_async_copy(src, staged.at[i], in_sem.at[i])
        for i, src in enumerate((adj_diag, alive_diag, adj_right, alive_right))
    ]
    load_k = pltpu.make_async_copy(truss_k, k_smem, k_sem)
    for load in loads:
        load.start()
    load_k.start()

    def at(offset):
        return lax.rem(me + offset + ndev, ndev)

    partners = [[] for _ in stages]
    for s, (stride, size) in enumerate(stages):
        place = lax.rem(me // stride, size)
        for k in range(1, size):
            partners[s].append(me + (lax.rem(place + k, size) - place) * stride)
    barrier = pltpu.get_barrier_semaphore()
    everyone = [at(o) for o in HALO] + sum(partners, [])
    for device in everyone:
        pl.semaphore_signal(barrier, inc=1, device_id=(device,), device_id_type=MESH)

    for load in loads:
        load.wait()
    mine[:words, :] = upper_words(staged[0] & staged[1])
    mine[words:, :] = staged[2] & staged[3]
    load_k.wait()
    thresh = (k_smem[0] - 2).astype(jnp.float32)

    dtype = wide.dtype

    def build_within(ref, slot):
        unpack(ref, wide.at[slot], dtype)
        upper = wide[slot].astype(jnp.float32)
        wide[slot] = (upper + upper.T).astype(dtype)

    build_within(mine.at[:words], 1)
    unpack(mine.at[words:], across.at[2], dtype)

    pl.semaphore_wait(barrier, len(everyone))
    copies = []
    for i, (offset, src, dst) in enumerate((
        (1, mine, near.at[0]),
        (-1, mine, near.at[1]),
        (2, mine.at[words:], far.at[0]),
        (-2, mine.at[:words], far.at[1]),
    )):
        copies.append(pltpu.make_async_remote_copy(
            src_ref=src, dst_ref=dst, send_sem=send_sem.at[i], recv_sem=recv_sem.at[i],
            device_id=(at(offset),), device_id_type=MESH,
        ))
        copies[-1].start()
    for copy in copies:
        copy.wait()
    build_within(near.at[0, :words], 0)
    unpack(near.at[0, words:], across.at[1], dtype)
    build_within(near.at[1, :words], 2)
    unpack(near.at[1, words:], across.at[3], dtype)
    unpack(far.at[0], across.at[0], dtype)
    build_within(far.at[1], 3)

    block = min(256, tile)
    ones = lambda x: jnp.sum(x, axis=0, keepdims=True)

    def lane_sum(x):
        return jnp.sum(x, axis=0, keepdims=True)

    def step_within(a_prev, w, a, new, final=False, count=False):
        before = after = 0
        for r in range(0, tile, block):
            rows = slice(r, r + block)
            s = dot(wide[w, rows, :], wide[w], 1, 0)
            s += dot(across[a, rows, :], across[a], 1, 1)
            s += dot(across[a_prev, :, rows], across[a_prev], 0, 0)
            old = wide[w, rows, :].astype(jnp.float32)
            kept = jnp.where(s >= thresh, old, 0.0)
            if final:
                support[rows, :tile] = s * kept
            else:
                wide[new, rows, :] = kept.astype(dtype)
            if count:
                before += lane_sum(old)
                after += lane_sum(kept)
        return before, after

    def step_across(w, a, w_next, new, final=False, count=False):
        before = after = 0
        for r in range(0, tile, block):
            rows = slice(r, r + block)
            s = dot(wide[w, rows, :], across[a], 1, 0)
            s += dot(across[a, rows, :], wide[w_next], 1, 0)
            old = across[a, rows, :].astype(jnp.float32)
            kept = jnp.where(s >= thresh, old, 0.0)
            if final:
                support[rows, tile:] = s * kept
            else:
                across[new, rows, :] = kept.astype(dtype)
            if count:
                before += lane_sum(old)
                after += lane_sum(kept)
        return before, after

    lost = []
    for j in range(3):
        b = step_within(j, j, j + 1, 4 + j, count=j == 1)
        c = step_across(j, j + 1, j + 1, 4 + j, count=j == 1)
        if j == 1:
            lost.append((b, c))
    for j in range(2):
        b = step_within(4 + j, 5 + j, 5 + j, 7 + j, count=j == 0)
        c = step_across(4 + j, 4 + j, 5 + j, 7 + j, count=j == 1)
        if j == 0:
            keep_b = b
    lost.append((keep_b, c))
    b = step_within(7, 7, 8, None, final=True, count=True)
    c = step_across(7, 8, 8, None, final=True, count=True)
    lost.append((b, c))

    lane = lax.broadcasted_iota(jnp.int32, (1, 128), 1)
    row = jnp.zeros((1, 128), jnp.int32)
    for i, ((b0, b1), (c0, c1)) in enumerate(lost):
        total = jnp.sum(0.5 * (b0 - b1) + (c0 - c1), axis=1, keepdims=True)
        row = jnp.where(lane == i, total.astype(jnp.int32), row)

    n = 0
    for s, (stride, size) in enumerate(stages):
        slots[s, 0:1, :] = row
        sends = []
        for k in range(1, size):
            sends.append(pltpu.make_async_remote_copy(
                src_ref=slots.at[s, 0:1], dst_ref=slots.at[s, k : k + 1],
                send_sem=sum_send.at[n], recv_sem=sum_recv.at[n],
                device_id=(partners[s][k - 1],), device_id_type=MESH,
            ))
            sends[-1].start()
            n += 1
        for send in sends:
            send.wait()
        row = jnp.sum(slots[s, :size, :], axis=0, keepdims=True)
    counts[...] = jnp.broadcast_to(row, counts.shape)


def on_device(ndev, *args):
    tile = args[0].shape[1]
    words = tile // WORD
    sums = sum(size - 1 for _, size in STAGES[ndev])
    vmem = pl.BlockSpec(memory_space=pltpu.VMEM)
    support, counts = pl.pallas_call(
        functools.partial(kernel, ndev, tile),
        out_shape=(
            jax.ShapeDtypeStruct((tile, 2 * tile), jnp.float32),
            jax.ShapeDtypeStruct((8, 128), jnp.int32),
        ),
        in_specs=[pl.BlockSpec(memory_space=pl.ANY)] * 5,
        out_specs=(vmem, vmem),
        scratch_shapes=[
            pltpu.VMEM((4, words, tile), jnp.int32),
            pltpu.SMEM((1,), jnp.int32),
            pltpu.VMEM((2 * words, tile), jnp.int32),
            pltpu.VMEM((2, 2 * words, tile), jnp.int32),
            pltpu.VMEM((2, words, tile), jnp.int32),
            pltpu.VMEM((9, tile, tile), jnp.bfloat16),
            pltpu.VMEM((9, tile, tile), jnp.bfloat16),
            pltpu.VMEM((len(STAGES[ndev]), 8, 128), jnp.int32),
            pltpu.SemaphoreType.DMA((4,)),
            pltpu.SemaphoreType.DMA,
            pltpu.SemaphoreType.DMA((4,)),
            pltpu.SemaphoreType.DMA((4,)),
            pltpu.SemaphoreType.DMA((sums,)),
            pltpu.SemaphoreType.DMA((sums,)),
        ],
        compiler_params=pltpu.CompilerParams(collective_id=0, has_side_effects=True),
        name="peel",
    )(*args)
    return support, counts[0, :3]


def solution(mesh):
    ndev = mesh.shape[AXIS]
    placed = (P(AXIS, None),) * 4 + (P(),)
    return jax.shard_map(
        functools.partial(on_device, ndev), mesh=mesh, in_specs=placed,
        out_specs=(P(AXIS, None), P()), check_vma=False,
    )
```
